512 devices in a mesh: ka: 256 (over y, z_lo, x, core), ga: 2 (over z_hi).
Axes of the slice: x: 4, y: 8, z: 8 (z_hi: 2, z_lo: 4; z = z_hi * 4 + z_lo), core: 2. Of those that a mesh axis runs over, the one named last changes fastest.
Arguments:
- pair_density: bfloat16 [2048, 32, 12032], P('ka', None, 'ga'), may hold values from -6 to 6
- coulomb: float32 [12032], P('ga'), may hold values from 3e-05 to 0.003
Outputs:
- kernel: float32 [65536, 1280], P(('ka', 'ga'))
The draws below stay inside these ranges and needn't reach their ends.
All inputs are finite; a program needn't handle non-finite values.
Results may differ from the reference program's by a relative error of at most 0.0013.
Values may be sent and summed in bfloat16 or wider, within the bound.
No kernel may reach another device: no remote copies, remote signals or barrier semaphores. Data moves between devices by JAX's collectives and lax.ppermute only.
A program may use at most 64 MiB of HBM per device.

```python
import math
import jax
import jax.numpy as jnp
from jax import lax

PAIRS = 32
G = 12032
K_DEV = 8
STEPS = 2
NK = 2048
N_KA = 256


def shard_levels(key, extent, cuts, least, high):
    gain = 1.0
    for axis_at, shards_of in cuts:
        draws = jax.random.uniform(jax.random.fold_in(jax.random.fold_in(key, 6), axis_at), (shards_of,), jnp.float32, least / len(cuts), high / len(cuts))
        gain = gain * jnp.repeat(jnp.exp(draws), extent[axis_at] // shards_of).reshape((-1,) + (1,) * (len(extent) - 1 - axis_at))
    return gain


def scatter_about(rng, shape, scale, most, split=(), kind=jnp.bfloat16):
    values = jax.random.normal(rng, shape, jnp.float32) * scale
    if len(split) > 0:
        values = shard_levels(rng, shape, split, -0.22, 0.18) * values
    return jnp.clip(values, min=-most, max=most).astype(kind)


def setup_inputs(seed: int = 0) -> dict:
    key_list = jax.random.split(jax.random.key(seed), 3)
    return {
        "pair_density": scatter_about(key_list[0], (NK, PAIRS, G), 1.0, 6.0, ((0, 256), (2, 2))),
        "coulomb": jnp.clip(jnp.exp(math.log(0.003) - 4.6051702 * jax.random.uniform(key_list[1], (G,), jnp.float32) ** shard_levels(key_list[1], (G,), ((0, 2),), -0.2, 0.2)), 2.9999999242136255e-05, 0.003),
    }


def reference(pair_density, coulomb):
    width = K_DEV * PAIRS
    density = pair_density.reshape(N_KA, width, G)

    def one_shard(index):
        own = lax.dynamic_index_in_dim(density, index, 0, False).astype(jnp.float32)
        weighted = lax.optimization_barrier((own * coulomb[None, :]).astype(jnp.bfloat16)).astype(jnp.float32)
        blocks = []
        for step in range(STEPS, -1, -1):
            other_index = ((index - step) % N_KA).astype(jnp.int32)
            other = lax.dynamic_index_in_dim(density, other_index, 0, False).astype(jnp.float32)
            blocks.append(jnp.dot(weighted, other.T, precision=lax.Precision.HIGHEST))
        return jnp.stack(blocks)

    lower = lax.map(one_shard, jnp.arange(N_KA, dtype=jnp.int32))
    columns = [lower[:, position] for position in range(STEPS + 1)]
    for step in range(1, STEPS + 1):
        mirrored = jnp.roll(lower[:, STEPS - step], -step, axis=0)
        columns.append(jnp.swapaxes(mirrored, 1, 2))
    joined = jnp.concatenate(columns, axis=2)
    return joined.reshape(N_KA * width, (2 * STEPS + 1) * width)
```

```python
import jax
import jax.numpy as jnp
from jax import lax
from jax.experimental import pallas as pl
from jax.experimental.pallas import tpu as pltpu
from jax.sharding import PartitionSpec as P

ROWS = 256
HALF = 128
EXTRA = 8
PEAK = 14.0

F32 = jnp.float32
BF16 = jnp.bfloat16
F16 = jnp.float16


def nt_dot(left, right):
    return lax.dot_general(left, right, (((1,), (1,)), ((), ())), preferred_element_type=F32)


def scale_rows(source, target, at, factor):
    def body(step, _):
        rows = pl.multiple_of(step * 16, 16)
        piece = source[pl.ds(rows, 16), :].astype(F32) * factor
        target[pl.ds(at + rows, 16), :] = piece.astype(BF16)
        return 0

    lax.fori_loop(0, ROWS // 16, body, 0)


def exponent_for(biggest):
    return PEAK - jnp.ceil(jnp.log2(jnp.maximum(biggest, 1e-30)))


def pack(message, block, exponent, columns):
    message[0:HALF, columns] = block * jnp.exp2(exponent)
    message[HALF : HALF + EXTRA, columns] = jnp.broadcast_to(exponent, (EXTRA, ROWS))


def unpack(message, columns):
    exponent = message[HALF : HALF + EXTRA, columns][0:1, :]
    return message[0:HALF, columns] * jnp.exp2(-exponent)


def sides(where_ref, coulomb_ref):
    even = where_ref[0] == 0
    weights = coulomb_ref[...]
    ones = jnp.ones_like(weights)
    return jnp.where(even, ones, weights), jnp.where(even, weights, ones)


def early_kernel(where_ref, coulomb_ref, own, sib, keep, message, left, weighted, acc):
    left_factor, right_factor = sides(where_ref, coulomb_ref)
    half = where_ref[1]
    mine = pl.multiple_of(half * HALF, HALF)
    other = pl.multiple_of((1 - half) * HALF, HALF)
    scale_rows(own, left, 0, left_factor)
    scale_rows(sib, left, ROWS, left_factor)
    scale_rows(own, weighted, 0, coulomb_ref[...])
    acc[:, 0:ROWS] = nt_dot(weighted[...], own[...])
    scale_rows(sib, weighted, 0, right_factor)
    acc[:, ROWS : 2 * ROWS] = nt_dot(left[0:ROWS, :], weighted[...])
    biggest = jnp.max(jnp.abs(acc[...]), axis=(0, 1), keepdims=True)
    exponent = exponent_for(biggest)
    keep[...] = acc[pl.ds(mine, HALF), :]
    for at in range(2):
        columns = slice(at * ROWS, (at + 1) * ROWS)
        pack(message, acc[pl.ds(other, HALF), columns], exponent, columns)


def late_kernel(where_ref, coulomb_ref, far, left, keep, to_sib, to_far, over, sib_over, far_over, weighted, acc, turned):
    _, right_factor = sides(where_ref, coulomb_ref)
    half = where_ref[1]
    mine = pl.multiple_of(half * HALF, HALF)
    other = pl.multiple_of((1 - half) * HALF, HALF)
    scale_rows(far, weighted, 0, right_factor)
    acc[...] = nt_dot(left[...], weighted[...])
    biggest = jnp.max(jnp.abs(acc[...]), axis=(0, 1), keepdims=True)
    exponent = exponent_for(biggest)
    turned[...] = acc[0:ROWS, :].T
    columns = slice(0, ROWS)
    keep[...] = acc[pl.ds(mine, HALF), :]
    pack(over, acc[pl.ds(other, HALF), :], exponent, columns)
    to_sib[...] = acc[pl.ds(ROWS + mine, HALF), :]
    pack(sib_over, acc[pl.ds(ROWS + other, HALF), :], exponent, columns)
    to_far[...] = turned[pl.ds(mine, HALF), :]
    pack(far_over, turned[pl.ds(other, HALF), :], exponent, columns)


def final_kernel(where_ref, early, early_over, keep, over, from_sib, sib_over, from_far, far_over, out):
    columns = slice(0, ROWS)
    nearest = early[:, 0:ROWS] + unpack(early_over, slice(0, ROWS))
    inside = early[:, ROWS : 2 * ROWS] + unpack(early_over, slice(ROWS, 2 * ROWS))
    outside = keep[...] + unpack(over, columns)
    beside = from_sib[...] + unpack(sib_over, columns)
    returned = from_far[...] + unpack(far_over, columns)
    order = [returned, beside, nearest, inside, outside]

    @pl.when(where_ref[0] == 0)
    def _():
        for at, block in enumerate(order):
            out[:, at * ROWS : (at + 1) * ROWS] = block

    @pl.when(where_ref[0] != 0)
    def _():
        for at, block in enumerate(reversed(order)):
            out[:, at * ROWS : (at + 1) * ROWS] = block


def vmem():
    return pl.BlockSpec(memory_space=pltpu.VMEM)


def smem():
    return pl.BlockSpec(memory_space=pltpu.SMEM)


def call(kernel, name, inputs, outputs, scratch):
    return pl.pallas_call(
        kernel,
        name=name,
        in_specs=[smem()] + [vmem()] * (inputs - 1),
        out_specs=[vmem()] * len(outputs),
        out_shape=[jax.ShapeDtypeStruct(shape, kind) for shape, kind in outputs],
        scratch_shapes=[pltpu.VMEM(shape, kind) for shape, kind in scratch],
        compiler_params=pltpu.CompilerParams(vmem_limit_bytes=56 * 1024 * 1024),
    )


def over_ga(value, pairs):
    count = lax.axis_size("ga")
    moves = [(s * count + h, t * count + 1 - h) for s, t in pairs for h in range(count)]
    return lax.ppermute(value.astype(F16), ("ka", "ga"), moves).astype(F32)


def shards(pair_density, coulomb):
    shard_points, pairs, waves = pair_density.shape
    width = shard_points * pairs
    count = lax.axis_size("ka")
    index = lax.axis_index("ka")
    half = lax.axis_index("ga")
    where = jnp.stack([index % 2, half]).astype(jnp.int32)
    same = [(i, i) for i in range(count)]
    swap = [(i, i ^ 1) for i in range(count)]
    send = [(i, (i - 2) % count if i % 2 == 0 else (i + 2) % count) for i in range(count)]
    back = [(t, s) for s, t in send]
    factor = coulomb.reshape(1, waves)

    far = lax.ppermute(pair_density, "ka", send).reshape(width, waves)
    sib = lax.ppermute(pair_density, "ka", swap).reshape(width, waves)
    own = pair_density.reshape(width, waves)
    early, early_msg, left = call(
        early_kernel,
        "early",
        4,
        [((HALF, 2 * ROWS), F32), ((HALF + EXTRA, 2 * ROWS), F32), ((2 * ROWS, waves), BF16)],
        [((ROWS, waves), BF16), ((ROWS, 2 * ROWS), F32)],
    )(where, factor, own, sib)
    early_over = over_ga(early_msg, same)
    keep, to_sib, to_far, over, sib_over, far_over = call(
        late_kernel,
        "late",
        4,
        [((HALF, ROWS), F32)] * 3 + [((HALF + EXTRA, ROWS), F32)] * 3,
        [((ROWS, waves), BF16), ((2 * ROWS, ROWS), F32), ((ROWS, ROWS), F32)],
    )(where, factor, far, left)
    far_over = over_ga(far_over, back)
    sib_over = over_ga(sib_over, swap)
    over = over_ga(over, same)
    from_far = lax.ppermute(to_far, "ka", back)
    from_sib = lax.ppermute(to_sib, "ka", swap)
    (out,) = call(final_kernel, "final", 9, [((HALF, 5 * ROWS), F32)], [])(
        where, early, early_over, keep, over, from_sib, sib_over, from_far, far_over
    )
    return out


def solution(mesh):
    in_specs = (P("ka", None, "ga"), P("ga"))
    out_specs = P(("ka", "ga"), None)
    return jax.shard_map(shards, mesh=mesh, in_specs=in_specs, out_specs=out_specs, check_vma=False)
```

```python
import jax
import jax.numpy as jnp
from jax import lax
from jax.experimental import pallas as pl
from jax.experimental.pallas import tpu as pltpu
from jax.sharding import PartitionSpec as P


ROWS = 256
HALF = 128
EXTRA = 8
PEAK = 14.0
STEP = 512

F32 = jnp.float32
BF16 = jnp.bfloat16
F16 = jnp.float16


def nt_dot(left, right):
    return lax.dot_general(left, right, (((1,), (1,)), ((), ())), preferred_element_type=F32)


def column_steps(waves):
    return [slice(at, min(at + STEP, waves)) for at in range(0, waves, STEP)]


def scaled(piece, factor):
    return (piece.astype(F32) * factor).astype(BF16)


def position():
    return lax.axis_index("ka") % 2 == 0, lax.axis_index("ga")


def exponent_for(biggest):
    return PEAK - jnp.ceil(jnp.log2(jnp.maximum(biggest, 1e-30)))


def send_exponent(message, exponent):
    message[HALF : HALF + EXTRA, :] = jnp.broadcast_to(exponent, (EXTRA, message.shape[1]))


def received(message, columns):
    return message[0:HALF, columns] * jnp.exp2(-message[HALF : HALF + 1, columns])


def early_kernel(coulomb, own, sib, keep, message, left):
    even, half = position()
    own_acc = jnp.zeros((ROWS, ROWS), F32)
    sib_acc = jnp.zeros((ROWS, ROWS), F32)
    for columns in column_steps(own.shape[1]):
        weight = coulomb[:, columns]
        ones = jnp.ones_like(weight)
        near = jnp.where(even, ones, weight)
        away = jnp.where(even, weight, ones)
        mine = own[:, columns]
        other = sib[:, columns]
        other_away = scaled(other, away)
        own_acc += nt_dot(scaled(mine, weight), mine)
        sib_acc += nt_dot(scaled(mine, near), other_away)
        left[0:ROWS, columns] = scaled(mine, away)
        left[ROWS : 2 * ROWS, columns] = other_away
    biggest = jnp.maximum(jnp.max(jnp.abs(own_acc)), jnp.max(jnp.abs(sib_acc)))
    exponent = exponent_for(jnp.full((1, 1), biggest))
    factor = jnp.exp2(exponent)
    send_exponent(message, exponent)
    for at, acc in ((0, own_acc), (ROWS, sib_acc)):
        columns = slice(at, at + ROWS)
        top, bottom = acc[0:HALF, :], acc[HALF:ROWS, :]
        keep[:, columns] = jnp.where(half == 0, top, bottom)
        message[0:HALF, columns] = jnp.where(half == 0, bottom, top) * factor


def late_kernel(coulomb, far, left, keep, across, corner, message):
    even, half = position()
    own_acc = jnp.zeros((ROWS, ROWS), F32)
    sib_acc = jnp.zeros((ROWS, ROWS), F32)
    for columns in column_steps(far.shape[1]):
        weight = coulomb[:, columns]
        ones = jnp.ones_like(weight)
        right = scaled(far[:, columns], jnp.where(even, ones, weight))
        own_acc += nt_dot(left[0:ROWS, columns], right)
        sib_acc += nt_dot(left[ROWS : 2 * ROWS, columns], right)
    biggest = jnp.maximum(jnp.max(jnp.abs(own_acc)), jnp.max(jnp.abs(sib_acc)))
    exponent = exponent_for(jnp.full((1, 1), biggest))
    factor = jnp.exp2(exponent)
    send_exponent(message, exponent)
    first = half == 0
    keep[...] = jnp.where(first, own_acc[0:HALF, :], own_acc[HALF:ROWS, :])
    message[0:HALF, 0:ROWS] = jnp.where(first, own_acc[HALF:ROWS, :], own_acc[0:HALF, :]) * factor
    mine = jnp.where(first, sib_acc[0:HALF, :], sib_acc[HALF:ROWS, :])
    other = jnp.where(first, sib_acc[HALF:ROWS, :], sib_acc[0:HALF, :])
    across[...] = mine
    corner[...] = jnp.where(first, other[:, 0:HALF], other[:, HALF:ROWS])
    message[0:HALF, ROWS : 2 * ROWS] = other * factor
    message[0:HALF, 2 * ROWS : 2 * ROWS + HALF] = (
        jnp.where(first, mine[:, HALF:ROWS], mine[:, 0:HALF]) * factor
    )


def sum_kernel(keep, across, corner, message, own_far, to_sib, to_far):
    _, half = position()
    first = half == 0
    own_far[...] = keep[...] + received(message, slice(0, ROWS))
    mine = across[...] + received(message, slice(ROWS, 2 * ROWS))
    to_sib[...] = mine
    other = (corner[...] + received(message, slice(2 * ROWS, 2 * ROWS + HALF))).T
    same = jnp.where(first, mine[:, 0:HALF], mine[:, HALF:ROWS]).T
    to_far[:, 0:HALF] = jnp.where(first, same, other)
    to_far[:, HALF:ROWS] = jnp.where(first, other, same)


def final_kernel(early, message, own_far, from_sib, from_far, out):
    even, _ = position()
    nearest = early[:, 0:ROWS] + received(message, slice(0, ROWS))
    inside = early[:, ROWS : 2 * ROWS] + received(message, slice(ROWS, 2 * ROWS))
    order = [from_far[...], own_far[...], nearest, inside, from_sib[...]]
    for at in range(5):
        out[:, at * ROWS : (at + 1) * ROWS] = jnp.where(even, order[at], order[4 - at])


def call(kernel, operands, outputs, on_chip=True):
    space = pltpu.MemorySpace.VMEM
    if on_chip:
        shapes = [space(shape, kind) for shape, kind in outputs]
    else:
        shapes = [jax.ShapeDtypeStruct(shape, kind) for shape, kind in outputs]
    return pl.pallas_call(
        kernel,
        in_specs=[pl.BlockSpec(memory_space=space)] * len(operands),
        out_specs=[pl.BlockSpec(memory_space=space)] * len(outputs),
        out_shape=shapes,
        compiler_params=pltpu.CompilerParams(vmem_limit_bytes=40 * 1024 * 1024),
    )(*[pltpu.with_memory_space_constraint(x, space) for x in operands])


def over_ga(value):
    return lax.ppermute(value.astype(F16), "ga", [(0, 1), (1, 0)]).astype(F32)


def shards(pair_density, coulomb):
    shard_points, pairs, waves = pair_density.shape
    width = shard_points * pairs
    count = lax.axis_size("ka")
    swap = [(i, i ^ 1) for i in range(count)]
    cross = [(i, (i - 1) % count if i % 2 == 0 else (i + 1) % count) for i in range(count)]
    factor = coulomb.reshape(1, waves)
    own = pair_density.reshape(width, waves)

    far = lax.ppermute(pair_density, "ka", cross)
    sib = lax.ppermute(pair_density, "ka", swap)
    far = far.reshape(width, waves)
    sib = sib.reshape(width, waves)
    early, early_message, left = call(
        early_kernel,
        (factor, own, sib),
        [((HALF, 2 * ROWS), F32), ((HALF + EXTRA, 2 * ROWS), F32), ((2 * ROWS, waves), BF16)],
    )
    early_message = over_ga(early_message)
    keep, across, corner, message = call(
        late_kernel,
        (factor, far, left),
        [
            ((HALF, ROWS), F32),
            ((HALF, ROWS), F32),
            ((HALF, HALF), F32),
            ((HALF + EXTRA, 2 * ROWS + HALF), F32),
        ],
    )
    own_far, to_sib, to_far = call(
        sum_kernel, (keep, across, corner, over_ga(message)), [((HALF, ROWS), F32)] * 3
    )
    from_far = lax.ppermute(to_far, "ka", cross)
    from_sib = lax.ppermute(to_sib, "ka", swap)
    (out,) = call(
        final_kernel,
        (early, early_message, own_far, from_sib, from_far),
        [((HALF, 5 * ROWS), F32)],
        on_chip=False,
    )
    return out


def solution(mesh):
    in_specs = (P("ka", None, "ga"), P("ga"))
    out_specs = P(("ka", "ga"), None)
    return jax.shard_map(shards, mesh=mesh, in_specs=in_specs, out_specs=out_specs, check_vma=False)
```

```python
import jax
import jax.numpy as jnp
from jax import lax
from jax.experimental import pallas as pl
from jax.experimental.pallas import tpu as pltpu
from jax.sharding import PartitionSpec as P


ROWS = 256
HALF = 128
EXTRA = 8
PEAK = 14.0
STEP = 512

F32 = jnp.float32
BF16 = jnp.bfloat16
F16 = jnp.float16


def nt_dot(left, right):
    return lax.dot_general(left, right, (((1,), (1,)), ((), ())), preferred_element_type=F32)


def column_steps(waves):
    return [slice(at, min(at + STEP, waves)) for at in range(0, waves, STEP)]


def scaled(piece, factor):
    return (piece.astype(F32) * factor).astype(BF16)


def position():
    return lax.axis_index("ka") % 2 == 0, lax.axis_index("ga")


def exponent_for(biggest):
    return PEAK - jnp.ceil(jnp.log2(jnp.maximum(biggest, 1e-30)))


def send_exponent(message, exponent):
    message[HALF : HALF + EXTRA, :] = jnp.broadcast_to(exponent, (EXTRA, message.shape[1]))


def received(message, columns):
    return message[0:HALF, columns] * jnp.exp2(-message[HALF : HALF + 1, columns])


def halves(block, half):
    top, bottom = block[0:HALF, :], block[HALF:ROWS, :]
    first = half == 0
    return jnp.where(first, top, bottom), jnp.where(first, bottom, top)


def early_kernel(coulomb, own, sib, keep, give, left):
    even, half = position()
    own_acc = jnp.zeros((ROWS, ROWS), F32)
    sib_acc = jnp.zeros((ROWS, ROWS), F32)
    for columns in column_steps(own.shape[1]):
        weight = coulomb[:, columns]
        ones = jnp.ones_like(weight)
        near = jnp.where(even, ones, weight)
        away = jnp.where(even, weight, ones)
        mine = own[:, columns]
        other = sib[:, columns]
        other_away = scaled(other, away)
        own_acc += nt_dot(scaled(mine, weight), mine)
        sib_acc += nt_dot(scaled(mine, near), other_away)
        left[0:ROWS, columns] = scaled(mine, away)
        left[ROWS : 2 * ROWS, columns] = other_away
    keep[:, 0:ROWS], give[:, 0:ROWS] = halves(own_acc, half)
    keep[:, ROWS : 2 * ROWS], give[:, ROWS : 2 * ROWS] = halves(sib_acc, half)


def across_kernel(coulomb, far, left, across, corner, message, right):
    even, half = position()
    acc = jnp.zeros((ROWS, ROWS), F32)
    for columns in column_steps(far.shape[1]):
        weight = coulomb[:, columns]
        piece = scaled(far[:, columns], jnp.where(even, jnp.ones_like(weight), weight))
        right[:, columns] = piece
        acc += nt_dot(left[ROWS : 2 * ROWS, columns], piece)
    exponent = exponent_for(jnp.full((1, 1), jnp.max(jnp.abs(acc))))
    factor = jnp.exp2(exponent)
    send_exponent(message, exponent)
    first = half == 0
    mine, other = halves(acc, half)
    across[...] = mine
    corner[...] = jnp.where(first, other[:, 0:HALF], other[:, HALF:ROWS])
    message[0:HALF, 0:ROWS] = other * factor
    message[0:HALF, ROWS : ROWS + HALF] = jnp.where(first, mine[:, HALF:ROWS], mine[:, 0:HALF]) * factor


def beside_kernel(right, left, give, keep, message):
    _, half = position()
    acc = nt_dot(left[0:ROWS, :], right[...])
    early = give[...]
    biggest = jnp.maximum(jnp.max(jnp.abs(acc)), jnp.max(jnp.abs(early)))
    exponent = exponent_for(jnp.full((1, 1), biggest))
    factor = jnp.exp2(exponent)
    send_exponent(message, exponent)
    keep[...], other = halves(acc, half)
    message[0:HALF, 0:ROWS] = other * factor
    message[0:HALF, ROWS : 3 * ROWS] = early * factor


def sum_kernel(across, corner, message, to_sib, to_far):
    _, half = position()
    first = half == 0
    mine = across[...] + received(message, slice(0, ROWS))
    other = (corner[...] + received(message, slice(ROWS, ROWS + HALF))).T
    same = jnp.where(first, mine[:, 0:HALF], mine[:, HALF:ROWS]).T
    biggest = jnp.maximum(jnp.max(jnp.abs(mine)), jnp.max(jnp.abs(other)))
    exponent = exponent_for(jnp.full((1, 1), biggest))
    factor = jnp.exp2(exponent)
    send_exponent(to_sib, exponent)
    send_exponent(to_far, exponent)
    to_sib[0:HALF, :] = mine * factor
    to_far[0:HALF, 0:HALF] = jnp.where(first, same, other) * factor
    to_far[0:HALF, HALF:ROWS] = jnp.where(first, other, same) * factor


def final_kernel(early, beside, message, from_sib, from_far, out):
    even, _ = position()
    own_far = beside[...] + received(message, slice(0, ROWS))
    nearest = early[:, 0:ROWS] + received(message, slice(ROWS, 2 * ROWS))
    inside = early[:, ROWS : 2 * ROWS] + received(message, slice(2 * ROWS, 3 * ROWS))
    whole = slice(0, ROWS)
    order = [received(from_far, whole), own_far, nearest, inside, received(from_sib, whole)]
    for at in range(5):
        out[:, at * ROWS : (at + 1) * ROWS] = jnp.where(even, order[at], order[4 - at])


def call(kernel, operands, outputs, on_chip=True):
    space = pltpu.MemorySpace.VMEM
    if on_chip:
        shapes = [space(shape, kind) for shape, kind in outputs]
    else:
        shapes = [jax.ShapeDtypeStruct(shape, kind) for shape, kind in outputs]
    return pl.pallas_call(
        kernel,
        in_specs=[pl.BlockSpec(memory_space=space)] * len(operands),
        out_specs=[pl.BlockSpec(memory_space=space)] * len(outputs),
        out_shape=shapes,
        compiler_params=pltpu.CompilerParams(vmem_limit_bytes=40 * 1024 * 1024),
    )(*[pltpu.with_memory_space_constraint(x, space) for x in operands])


def sent(value, axes, pairs):
    return lax.ppermute(value.astype(F16), axes, pairs).astype(F32)


def over_ga(value):
    return sent(value, "ga", [(0, 1), (1, 0)])


def shards(pair_density, coulomb):
    shard_points, pairs, waves = pair_density.shape
    width = shard_points * pairs
    count = lax.axis_size("ka")
    swap = [(i, i ^ 1) for i in range(count)]
    cross = [(i, (i - 1) % count if i % 2 == 0 else (i + 1) % count) for i in range(count)]
    factor = coulomb.reshape(1, waves)
    own = pair_density.reshape(width, waves)

    far = lax.ppermute(pair_density, "ka", cross)
    sib = lax.ppermute(pair_density, "ka", swap)
    far = far.reshape(width, waves)
    sib = sib.reshape(width, waves)
    early, give, left = call(
        early_kernel,
        (factor, own, sib),
        [((HALF, 2 * ROWS), F32), ((HALF, 2 * ROWS), F32), ((2 * ROWS, waves), BF16)],
    )
    across, corner, message, right = call(
        across_kernel,
        (factor, far, left),
        [
            ((HALF, ROWS), F32),
            ((HALF, HALF), F32),
            ((HALF + EXTRA, ROWS + HALF), F32),
            ((ROWS, waves), BF16),
        ],
    )
    message = over_ga(message)
    beside, rest = call(
        beside_kernel, (right, left, give), [((HALF, ROWS), F32), ((HALF + EXTRA, 3 * ROWS), F32)]
    )
    rest = over_ga(rest)
    to_sib, to_far = call(sum_kernel, (across, corner, message), [((HALF + EXTRA, ROWS), F32)] * 2)
    from_far = sent(to_far, "ka", cross)
    from_sib = sent(to_sib, "ka", swap)
    (out,) = call(
        final_kernel,
        (early, beside, rest, from_sib, from_far),
        [((HALF, 5 * ROWS), F32)],
        on_chip=False,
    )
    return out


def solution(mesh):
    in_specs = (P("ka", None, "ga"), P("ga"))
    out_specs = P(("ka", "ga"), None)
    return jax.shard_map(shards, mesh=mesh, in_specs=in_specs, out_specs=out_specs, check_vma=False)
```

```python
import jax
import jax.numpy as jnp
from jax import lax
from jax.experimental import pallas as pl
from jax.experimental.pallas import tpu as pltpu
from jax.sharding import PartitionSpec as P


ROWS = 256
HALF = 128
EXTRA = 8
PEAK = 14.0
STEP = 512

F32 = jnp.float32
BF16 = jnp.bfloat16
F16 = jnp.float16


def nt_dot(left, right):
    return lax.dot_general(left, right, (((1,), (1,)), ((), ())), preferred_element_type=F32)


def column_steps(waves):
    return [slice(at, min(at + STEP, waves)) for at in range(0, waves, STEP)]


def scaled(piece, factor):
    return (piece.astype(F32) * factor).astype(BF16)


def position():
    return lax.axis_index("ka") % 2 == 0, lax.axis_index("ga")


def exponent_for(biggest):
    return PEAK - jnp.ceil(jnp.log2(jnp.maximum(biggest, 1e-30)))


def common_exponent(given, message):
    return jnp.minimum(given[HALF : HALF + 1, 0:1], message[HALF : HALF + 1, 0:1])


def send_exponent(message, exponent):
    message[HALF : HALF + EXTRA, :] = jnp.broadcast_to(exponent, (EXTRA, message.shape[1]))


def received(message, columns):
    return message[0:HALF, columns] * jnp.exp2(-message[HALF : HALF + 1, columns])


def halves(block, half):
    top, bottom = block[0:HALF, :], block[HALF:ROWS, :]
    first = half == 0
    return jnp.where(first, top, bottom), jnp.where(first, bottom, top)


def early_kernel(coulomb, own, sib, keep, give, left):
    even, half = position()
    own_acc = jnp.zeros((ROWS, ROWS), F32)
    sib_acc = jnp.zeros((ROWS, ROWS), F32)
    for columns in column_steps(own.shape[1]):
        weight = coulomb[:, columns]
        ones = jnp.ones_like(weight)
        near = jnp.where(even, ones, weight)
        away = jnp.where(even, weight, ones)
        mine = own[:, columns]
        other = sib[:, columns]
        other_away = scaled(other, away)
        own_acc += nt_dot(scaled(mine, weight), mine)
        sib_acc += nt_dot(scaled(mine, near), other_away)
        left[0:ROWS, columns] = scaled(mine, away)
        left[ROWS : 2 * ROWS, columns] = other_away
    keep[:, 0:ROWS], give[:, 0:ROWS] = halves(own_acc, half)
    keep[:, ROWS : 2 * ROWS], give[:, ROWS : 2 * ROWS] = halves(sib_acc, half)


def across_kernel(coulomb, far, left, across, corner, message):
    even, half = position()
    acc = jnp.zeros((ROWS, ROWS), F32)
    for columns in column_steps(far.shape[1]):
        weight = coulomb[:, columns]
        piece = scaled(far[:, columns], jnp.where(even, jnp.ones_like(weight), weight))
        acc += nt_dot(left[ROWS : 2 * ROWS, columns], piece)
    exponent = exponent_for(jnp.full((1, 1), jnp.max(jnp.abs(acc))))
    factor = jnp.exp2(exponent)
    send_exponent(message, exponent)
    first = half == 0
    mine, other = halves(acc, half)
    across[...] = mine
    corner[...] = jnp.where(first, other[:, 0:HALF], other[:, HALF:ROWS])
    message[0:HALF, 0:ROWS] = other * factor
    message[0:HALF, ROWS : ROWS + HALF] = jnp.where(first, mine[:, HALF:ROWS], mine[:, 0:HALF]) * factor


def beside_kernel(coulomb, far, left, give, keep, message):
    even, half = position()
    acc = jnp.zeros((ROWS, ROWS), F32)
    for columns in column_steps(far.shape[1]):
        weight = coulomb[:, columns]
        piece = scaled(far[:, columns], jnp.where(even, jnp.ones_like(weight), weight))
        acc += nt_dot(left[0:ROWS, columns], piece)
    early = give[...]
    biggest = jnp.maximum(jnp.max(jnp.abs(acc)), jnp.max(jnp.abs(early)))
    exponent = exponent_for(jnp.full((1, 1), biggest))
    factor = jnp.exp2(exponent)
    send_exponent(message, exponent)
    keep[...], other = halves(acc, half)
    message[0:HALF, 0:ROWS] = other * factor
    message[0:HALF, ROWS : 3 * ROWS] = early * factor


def sum_kernel(across, corner, given, message, to_sib, to_far):
    _, half = position()
    first = half == 0
    mine = across[...] + received(message, slice(0, ROWS))
    other = (corner[...] + received(message, slice(ROWS, ROWS + HALF))).T
    same = jnp.where(first, mine[:, 0:HALF], mine[:, HALF:ROWS]).T
    exponent = common_exponent(given, message)
    factor = jnp.exp2(exponent)
    send_exponent(to_sib, exponent)
    send_exponent(to_far, exponent)
    to_sib[0:HALF, :] = mine * factor
    to_far[0:HALF, 0:HALF] = jnp.where(first, same, other) * factor
    to_far[0:HALF, HALF:ROWS] = jnp.where(first, other, same) * factor


def middle_kernel(early, beside, message, out, blocks, done):
    even, _ = position()
    own_far = beside[...] + received(message, slice(0, ROWS))
    inside = early[:, ROWS : 2 * ROWS] + received(message, slice(2 * ROWS, 3 * ROWS))
    blocks[:, 0:ROWS] = jnp.where(even, own_far, inside)
    blocks[:, ROWS : 2 * ROWS] = early[:, 0:ROWS] + received(message, slice(ROWS, 2 * ROWS))
    blocks[:, 2 * ROWS : 3 * ROWS] = jnp.where(even, inside, own_far)
    copy = pltpu.make_async_copy(blocks, out.at[:, ROWS : 4 * ROWS], done)
    copy.start()
    copy.wait()


def ends_kernel(from_sib, from_far, filled, out, low, high, low_done, high_done):
    del filled
    even, _ = position()
    whole = slice(0, ROWS)
    sib_block = received(from_sib, whole)
    far_block = received(from_far, whole)
    low[...] = jnp.where(even, far_block, sib_block)
    low_copy = pltpu.make_async_copy(low, out.at[:, 0:ROWS], low_done)
    low_copy.start()
    high[...] = jnp.where(even, sib_block, far_block)
    high_copy = pltpu.make_async_copy(high, out.at[:, 4 * ROWS : 5 * ROWS], high_done)
    high_copy.start()
    low_copy.wait()
    high_copy.wait()


def call(kernel, operands, outputs):
    space = pltpu.MemorySpace.VMEM
    return pl.pallas_call(
        kernel,
        in_specs=[pl.BlockSpec(memory_space=space)] * len(operands),
        out_specs=[pl.BlockSpec(memory_space=space)] * len(outputs),
        out_shape=[space(shape, kind) for shape, kind in outputs],
        compiler_params=pltpu.CompilerParams(vmem_limit_bytes=40 * 1024 * 1024),
    )(*[pltpu.with_memory_space_constraint(x, space) for x in operands])


def write_out(kernel, operands, widths, filled=None):
    space = pltpu.MemorySpace.VMEM
    held = [pltpu.with_memory_space_constraint(x, space) for x in operands]
    specs = [pl.BlockSpec(memory_space=space)] * len(held)
    aliases = {}
    if filled is not None:
        aliases = {len(held): 0}
        held.append(filled)
        specs.append(pl.BlockSpec(memory_space=pl.ANY))
    return pl.pallas_call(
        kernel,
        in_specs=specs,
        out_specs=pl.BlockSpec(memory_space=pl.ANY),
        out_shape=jax.ShapeDtypeStruct((HALF, 5 * ROWS), F32),
        scratch_shapes=[pltpu.VMEM((HALF, width), F32) for width in widths]
        + [pltpu.SemaphoreType.DMA] * len(widths),
        input_output_aliases=aliases,
    )(*held)


def sent(value, axes, pairs):
    return lax.ppermute(value.astype(F16), axes, pairs).astype(F32)


def over_ga(value):
    return sent(value, "ga", [(0, 1), (1, 0)])


def shards(pair_density, coulomb):
    shard_points, pairs, waves = pair_density.shape
    width = shard_points * pairs
    count = lax.axis_size("ka")
    swap = [(i, i ^ 1) for i in range(count)]
    cross = [(i, (i - 1) % count if i % 2 == 0 else (i + 1) % count) for i in range(count)]
    factor = coulomb.reshape(1, waves)
    own = pair_density.reshape(width, waves)

    far = lax.ppermute(pair_density, "ka", cross)
    sib = lax.ppermute(pair_density, "ka", swap)
    far = far.reshape(width, waves)
    sib = sib.reshape(width, waves)
    early, give, left = call(
        early_kernel,
        (factor, own, sib),
        [((HALF, 2 * ROWS), F32), ((HALF, 2 * ROWS), F32), ((2 * ROWS, waves), BF16)],
    )
    across, corner, message = call(
        across_kernel,
        (factor, far, left),
        [
            ((HALF, ROWS), F32),
            ((HALF, HALF), F32),
            ((HALF + EXTRA, ROWS + HALF), F32),
        ],
    )
    taken = over_ga(message)
    beside, rest = call(
        beside_kernel,
        (factor, far, left, give),
        [((HALF, ROWS), F32), ((HALF + EXTRA, 3 * ROWS), F32)],
    )
    rest = over_ga(rest)
    to_sib, to_far = call(
        sum_kernel, (across, corner, message, taken), [((HALF + EXTRA, ROWS), F32)] * 2
    )
    from_far = sent(to_far, "ka", cross)
    from_sib = sent(to_sib, "ka", swap)
    out = write_out(middle_kernel, (early, beside, rest), (3 * ROWS,))
    return write_out(ends_kernel, (from_sib, from_far), (ROWS, ROWS), out)


def solution(mesh):
    in_specs = (P("ka", None, "ga"), P("ga"))
    out_specs = P(("ka", "ga"), None)
    return jax.shard_map(shards, mesh=mesh, in_specs=in_specs, out_specs=out_specs, check_vma=False)
```
